256 devices in a mesh: span: 256 (over x, y, z, core).
Axes of the slice: x: 4, y: 4, z: 8, core: 2. Of those that a mesh axis runs over, the one named last changes fastest.
Arguments:
- random_slabs: bfloat16 [8192, 4, 3, 2048], P('span'), may hold values from -6 to 6
- span_weights: float32 [513], replicated, may hold values from 0.1 to 2
- wall_filter: bfloat16 [2048, 2048], replicated, may hold values from -0.125 to 0.125
- prev_state: float32 [8192, 3, 2048], P('span'), may hold values from -6 to 6
- time_scale: float32 [3, 2048], replicated, may hold values from 1 to 32
- mean_velocity: float32 [2048], replicated, may hold values from 0 to 2
- lund_diag: float32 [3, 2048], replicated, may hold values from 0.3 to 3
- lund_off: float32 [3, 2048], replicated, may hold values from -1 to 1
Outputs:
- velocity: bfloat16 [8192, 4, 3, 2048], P('span')
- new_state: float32 [8192, 3, 2048], P('span')
The draws below stay inside these ranges and needn't reach their ends.
All inputs are finite; a program needn't handle non-finite values.
Results may differ from the reference program's by a relative error of at most 0.0051.
Values may be sent and summed in bfloat16 or wider, within the bound.
A program may use at most 128 MiB of HBM per device.

```python
import math
import jax
import jax.numpy as jnp
from jax import lax

NY = 2048
PLANES = 4
NZ = 8192
HALF = 256


def draw_span_weights(key, part):
    offsets = jnp.arange(-HALF, HALF + 1).astype(jnp.float32)
    spread = jnp.float32(HALF)
    envelope = jnp.exp(-jnp.pi * offsets * offsets / (2.0 * spread * spread))
    factor = jnp.exp(jax.random.uniform(key, (2 * HALF + 1,), jnp.float32, math.log(0.5), math.log(2.0)))
    return envelope * factor


def steps_of(rng, shape, cuts, smallest, top_value):
    factor_of, own = 1.0, jax.random.fold_in(rng, 6)
    for position, shards_of in cuts:
        steps = jnp.exp(jax.random.uniform(jax.random.fold_in(own, position), (shards_of,), jnp.float32, smallest / len(cuts), top_value / len(cuts)))
        factor_of = factor_of * jnp.repeat(steps, shape[position] // shards_of).reshape([-1 if axis == position else 1 for axis in range(len(shape))])
    return factor_of


def bell_draw(rng, extent, scale, bound, shards=(), kind=jnp.bfloat16):
    level = steps_of(rng, extent, shards, -0.22, 0.18) if shards else 1.0
    result = jax.random.normal(rng, extent, jnp.float32) * scale * level
    return jnp.minimum(jnp.maximum(result, -bound), bound).astype(kind)


def setup_inputs(seed: int = 0) -> dict:
    key_list = jax.random.split(jax.random.key(seed), 9)
    return {
        "random_slabs": bell_draw(key_list[0], (NZ, PLANES, 3, NY), 1.0, 6.0, ((0, 256),)),
        "span_weights": draw_span_weights(jax.random.fold_in(key_list[8], 71), 0),
        "wall_filter": bell_draw(key_list[2], (NY, NY), NY ** -0.5, 0.125),
        "prev_state": bell_draw(key_list[3], (NZ, 3, NY), 1.0, 6.0, ((0, 256),), jnp.float32),
        "time_scale": jnp.clip(jnp.exp(jax.random.uniform(key_list[4], (3, NY), jnp.float32, math.log(1.0), math.log(32.0))), 1.0, 32.0),
        "mean_velocity": jnp.clip(jax.random.uniform(key_list[5], (NY,), jnp.float32, 0.0, 2.0), 0.0, 2.0),
        "lund_diag": jnp.clip(jnp.exp(jax.random.uniform(key_list[6], (3, NY), jnp.float32, math.log(0.3), math.log(3.0))), 0.3, 3.0),
        "lund_off": jnp.clip(jax.random.uniform(key_list[7], (3, NY), jnp.float32, -1.0, 1.0), -1.0, 1.0),
    }


def normalized_taps(span_weights):
    norm = jnp.sqrt(jnp.sum(span_weights * span_weights))
    return (span_weights / norm).astype(jnp.bfloat16)

def reference(random_slabs, span_weights, wall_filter, prev_state, time_scale, mean_velocity, lund_diag, lund_off):
    total = random_slabs.shape[0]
    taps = lax.optimization_barrier(normalized_taps(span_weights)).astype(jnp.float32)
    middle = jnp.zeros((total - 2 * HALF - 1,), jnp.float32)
    kernel = jnp.concatenate([taps[HALF:], middle, taps[:HALF]])
    kernel_hat = jnp.conj(jnp.fft.rfft(kernel))
    slabs = random_slabs.reshape(total, PLANES * 3, NY).transpose(1, 0, 2)
    wall_wide = wall_filter.astype(jnp.float32)

    def one_slab(slab):
        spectrum = jnp.fft.rfft(slab.astype(jnp.float32), axis=0)
        spanned = jnp.fft.irfft(spectrum * kernel_hat[:, None], n=total, axis=0)
        spanned = lax.optimization_barrier(spanned.astype(jnp.bfloat16)).astype(jnp.float32)
        return jnp.dot(spanned, wall_wide.T, precision=lax.Precision.HIGHEST)
    filtered = lax.map(one_slab, slabs).reshape(PLANES, 3, total, NY)
    decay = jnp.exp(-jnp.pi / (2.0 * time_scale))[:, None, :]
    inject = jnp.sqrt(1.0 - jnp.exp(-jnp.pi / time_scale))[:, None, :]

    def advance(state, plane):
        state = decay * state + inject * plane
        return (state, state)
    final, fluct = lax.scan(advance, prev_state.transpose(1, 0, 2), filtered)
    along = fluct[:, 0]
    normal = fluct[:, 1]
    spanwise = fluct[:, 2]
    first = mean_velocity + lund_diag[0] * along
    second = lund_off[0] * along + lund_diag[1] * normal
    third = lund_off[1] * along + lund_off[2] * normal + lund_diag[2] * spanwise
    velocity = jnp.stack([first, second, third], axis=1).astype(jnp.bfloat16)
    return (velocity.transpose(2, 0, 1, 3), final.transpose(1, 0, 2))
```

```python
import jax
import jax.numpy as jnp
from jax import lax
from jax.experimental import pallas as pl
from jax.experimental.pallas import tpu as pltpu
from jax.sharding import PartitionSpec as P

MESH = pl.DeviceIdType.MESH
GROUP = 16
ROWS = 32
LANES = 128
HALF = 256
PEERS = [(0, 1)] + [(sign * far, other) for far in (1, 2, 3) for sign in (1, -1) for other in (0, 1)] + [(4, 0), (4, 1)]


def slot_of(far, other):
    return (far % 8) * 2 + other


def kernel(
    x, wall, prev, weights, scale, mean, diag, off,
    velocity, final,
    held, spread, columns, made, spanned, wide, turned, band, state, carried, sums, moving, mixed, shown,
    vweights, vscale, vmean, vdiag, voff,
    in_send, in_recv, halo_send, halo_recv, out_send, out_recv, load_sem, own_sem, store_sem,
):
    devices = lax.axis_size("span")
    me = lax.axis_index("span")
    base = (me // GROUP) * GROUP
    pos = lax.rem(me, GROUP)
    chip = pos // 2
    core = lax.rem(pos, 2)

    def place(far, other):
        return lax.rem(chip + far + 8, 8) * 2 + lax.rem(core + other, 2)

    before = lax.rem(me + devices - GROUP, devices)
    after = lax.rem(me + GROUP, devices)

    loads = []
    for index, (source, target) in enumerate(
        ((weights, vweights), (scale, vscale), (mean, vmean), (diag, vdiag), (off, voff), (prev, state), (wall, wide))
    ):
        loads.append(pltpu.make_async_copy(source, target, load_sem.at[index]))
        loads[-1].start()
    own = []
    for c in range(3):
        own.append(
            pltpu.make_async_copy(
                x.at[:, c, :, pl.ds(pl.multiple_of(pos * LANES, LANES), LANES)], held.at[c, 8 + pos], own_sem.at[c]
            )
        )
        own[-1].start()

    barrier = pltpu.get_barrier_semaphore()
    for far, other in PEERS:
        pl.semaphore_signal(barrier, inc=1, device_id=(base + place(far, other),), device_id_type=MESH)
    for device in (before, after):
        pl.semaphore_signal(barrier, inc=1, device_id=(device,), device_id_type=MESH)
    pl.semaphore_wait(barrier, len(PEERS) + 2)

    arriving = []
    for c in range(3):
        arriving.append([])
        for far, other in PEERS:
            there = place(far, other)
            slot = slot_of(far, other)
            arriving[c].append(
                pltpu.make_async_remote_copy(
                    src_ref=x.at[:, c, :, pl.ds(pl.multiple_of(there * LANES, LANES), LANES)],
                    dst_ref=held.at[c, 8 + pos],
                    send_sem=in_send.at[c, slot],
                    recv_sem=in_recv.at[c, slot],
                    device_id=(base + there,),
                    device_id_type=MESH,
                )
            )
            arriving[c][-1].start()

    loads[0].wait()
    taps = vweights[...]
    taps = (taps / jnp.sqrt(jnp.sum(taps * taps))).astype(jnp.bfloat16).astype(jnp.float32)
    padded = jnp.concatenate([taps, jnp.zeros((1, 1024 - taps.shape[1]), jnp.float32)], axis=1)
    rolled = pltpu.roll(jnp.broadcast_to(padded, (HALF, 1024)), 0, 1, stride=1, stride_axis=0)
    band[...] = rolled[:, : 3 * HALF].astype(jnp.bfloat16)

    loads[6].wait()
    one = (
        lax.broadcasted_iota(jnp.int32, (256, 256), 0) == lax.broadcasted_iota(jnp.int32, (256, 256), 1)
    ).astype(jnp.bfloat16)

    def turn(step, carry):
        row = pl.multiple_of(step * 256, 256)
        for block in range(8):
            piece = wide[pl.ds(row, 256), block * 256 : (block + 1) * 256]
            turned[block * 256 : (block + 1) * 256, pl.ds(row, 256)] = lax.dot_general(
                one, piece, (((1,), (1,)), ((), ())), preferred_element_type=jnp.float32
            ).astype(jnp.bfloat16)
        return carry

    lax.fori_loop(0, 8, turn, 0)

    for index in range(1, 6):
        loads[index].wait()

    flat = held.reshape(3 * 32 * ROWS * 4, LANES)

    def unpack(c, slot):
        first = pl.multiple_of((c * 32 + slot) * LANES, LANES)
        row = pl.multiple_of(slot * LANES, LANES)
        spread[pl.ds(row, LANES), :] = flat[pl.ds(first, LANES), :].astype(jnp.float32)
        for t in range(4):
            columns[pl.ds(pl.multiple_of(slot * ROWS, ROWS), ROWS), t * LANES : (t + 1) * LANES] = spread[
                pl.ds(row + t, ROWS, stride=4), :
            ].astype(jnp.bfloat16)

    halos = []
    leaving = []
    for c in range(3):
        own[c].wait()
        for copy in arriving[c]:
            copy.wait_recv()
        halos.append([])
        for index, (source, target, device) in enumerate(((8, 24, before), (16, 0, after))):
            halos[c].append(
                pltpu.make_async_remote_copy(
                    src_ref=held.at[c, pl.ds(source, 8)],
                    dst_ref=held.at[c, pl.ds(target, 8)],
                    send_sem=halo_send.at[c, index],
                    recv_sem=halo_recv.at[c, index],
                    device_id=(device,),
                    device_id_type=MESH,
                )
            )
            halos[c][-1].start()

        def middle(step, carry):
            for part in range(4):
                unpack(c, 8 + step * 4 + part)
            return carry

        lax.fori_loop(0, 4, middle, 0)
        for copy in halos[c]:
            copy.wait_recv()

        def outer(step, carry):
            for part in range(4):
                unpack(c, step * 4 + part)
                unpack(c, 24 + step * 4 + part)
            return carry

        lax.fori_loop(0, 2, outer, 0)
        for half in range(2):
            block = jnp.dot(
                band[...], columns[half * HALF : half * HALF + 3 * HALF, :], preferred_element_type=jnp.float32
            ).astype(jnp.bfloat16)
            for t in range(4):
                made[c, t, half * HALF : (half + 1) * HALF, :] = block[:, t * LANES : (t + 1) * LANES]
        spanned[c, :, :, pl.ds(pl.multiple_of(pos * LANES, LANES), LANES)] = made[
            c, :, pl.ds(pl.multiple_of(pos * ROWS, ROWS), ROWS), :
        ]
        leaving.append([])
        for far, other in PEERS:
            there = place(far, other)
            slot = slot_of(far, other)
            leaving[c].append(
                pltpu.make_async_remote_copy(
                    src_ref=made.at[c, :, pl.ds(pl.multiple_of(there * ROWS, ROWS), ROWS), :],
                    dst_ref=spanned.at[c, :, :, pl.ds(pl.multiple_of(pos * LANES, LANES), LANES)],
                    send_sem=out_send.at[c, slot],
                    recv_sem=out_recv.at[c, slot],
                    device_id=(base + there,),
                    device_id_type=MESH,
                )
            )
            leaving[c][-1].start()

    stores = []
    for c in range(3):
        for index, far in enumerate((0, 1, -1, 2, -2, 3, -3, 4)):
            for copy, peer in zip(leaving[c], PEERS):
                if peer[0] == far:
                    copy.wait_recv()
            origin = pl.multiple_of(lax.rem(chip - far + 8, 8) * 256, 256)
            piece = spanned[c, :, :, pl.ds(origin, 256)].reshape(4 * ROWS, 256)
            term = jnp.dot(piece, turned[pl.ds(origin, 256), :], preferred_element_type=jnp.float32)
            if index == 0:
                sums[...] = term
            else:
                sums[...] += term
        for block in range(8):
            cols = slice(block * 256, (block + 1) * 256)
            time = vscale[c : c + 1, cols]
            decay = jnp.exp(-jnp.pi / (2.0 * time))
            inject = jnp.sqrt(1.0 - jnp.exp(-jnp.pi / time))
            value = state[c, :, cols]
            for t in range(4):
                value = decay * value + inject * sums[t * ROWS : (t + 1) * ROWS, cols]
                if c == 0:
                    carried[0, t, :, cols] = value
                    out = vmean[:, cols] + vdiag[0:1, cols] * value
                elif c == 1:
                    along = carried[0, t, :, cols]
                    out = voff[0:1, cols] * along + vdiag[1:2, cols] * value
                    carried[0, t, :, cols] = voff[1:2, cols] * along + voff[2:3, cols] * value
                else:
                    out = carried[0, t, :, cols] + vdiag[2:3, cols] * value
                for side in range(2):
                    mixed[2 * block + side, pl.ds(t, ROWS, stride=4), :] = out[:, side * LANES : (side + 1) * LANES]
            shown[c, :, cols] = value
            for tile in (2 * block, 2 * block + 1):
                moving[c, :, :, tile * LANES : (tile + 1) * LANES] = (
                    mixed[tile].reshape(ROWS, 4, LANES).astype(jnp.bfloat16)
                )
        stores.append(pltpu.make_async_copy(shown.at[c], final.at[c], store_sem.at[0, c]))
        stores[-1].start()
        stores.append(pltpu.make_async_copy(moving.at[c], velocity.at[:, c], store_sem.at[1, c]))
        stores[-1].start()

    for c in range(3):
        for copy in arriving[c] + halos[c] + leaving[c]:
            copy.wait_send()
    for copy in stores:
        copy.wait()


def body(random_slabs, span_weights, wall_filter, prev_state, time_scale, mean_velocity, lund_diag, lund_off):
    rows, planes, parts, width = random_slabs.shape
    any_spec = pl.BlockSpec(memory_space=pl.ANY)
    bf16, f32 = jnp.bfloat16, jnp.float32
    velocity, state = pl.pallas_call(
        kernel,
        out_shape=(
            jax.ShapeDtypeStruct((rows, parts, planes, width), bf16),
            jax.ShapeDtypeStruct((parts, rows, width), f32),
        ),
        in_specs=[any_spec] * 8,
        out_specs=(any_spec, any_spec),
        scratch_shapes=[
            pltpu.VMEM((3, 32, ROWS, 4, LANES), bf16),
            pltpu.VMEM((4096, LANES), f32),
            pltpu.VMEM((1024, 4 * LANES), bf16),
            pltpu.VMEM((3, 4, 512, LANES), bf16),
            pltpu.VMEM((3, 4, ROWS, width), bf16),
            pltpu.VMEM((width, width), bf16),
            pltpu.VMEM((width, width), bf16),
            pltpu.VMEM((HALF, 3 * HALF), bf16),
            pltpu.VMEM((3, ROWS, width), f32),
            pltpu.VMEM((1, 4, ROWS, width), f32),
            pltpu.VMEM((4 * ROWS, width), f32),
            pltpu.VMEM((3, ROWS, 4, width), bf16),
            pltpu.VMEM((width // LANES, 4 * ROWS, LANES), f32),
            pltpu.VMEM((3, ROWS, width), f32),
            pltpu.VMEM((1, 2 * HALF + 1), f32),
            pltpu.VMEM((3, width), f32),
            pltpu.VMEM((1, width), f32),
            pltpu.VMEM((3, width), f32),
            pltpu.VMEM((3, width), f32),
            pltpu.SemaphoreType.DMA((3, 16)),
            pltpu.SemaphoreType.DMA((3, 16)),
            pltpu.SemaphoreType.DMA((3, 2)),
            pltpu.SemaphoreType.DMA((3, 2)),
            pltpu.SemaphoreType.DMA((3, 16)),
            pltpu.SemaphoreType.DMA((3, 16)),
            pltpu.SemaphoreType.DMA((7,)),
            pltpu.SemaphoreType.DMA((3,)),
            pltpu.SemaphoreType.DMA((2, 3)),
        ],
        compiler_params=pltpu.CompilerParams(collective_id=0, has_side_effects=True, vmem_limit_bytes=60 * 2**20),
        name="inflow",
    )(
        random_slabs.transpose(0, 2, 1, 3),
        wall_filter,
        prev_state.transpose(1, 0, 2),
        span_weights.reshape(1, -1),
        time_scale,
        mean_velocity.reshape(1, -1),
        lund_diag,
        lund_off,
    )
    return velocity.transpose(0, 2, 1, 3), state.transpose(1, 0, 2)


def solution(mesh):
    placed = (P("span", None, None, None), P(), P(), P("span", None, None), P(), P(), P(), P())
    return jax.shard_map(
        body,
        mesh=mesh,
        in_specs=placed,
        out_specs=(P("span", None, None, None), P("span", None, None)),
        check_vma=False,
    )
```

```python
import jax
import jax.numpy as jnp
from jax import lax
from jax.experimental import pallas as pl
from jax.experimental.pallas import tpu as pltpu
from jax.sharding import PartitionSpec as P

MESH = pl.DeviceIdType.MESH
GROUP = 16
ROWS = 32
LANES = 128
HALF = 256
PEERS = [(0, 1)] + [(sign * far, other) for far in (1, 2, 3) for sign in (1, -1) for other in (0, 1)] + [(4, 0), (4, 1)]


def slot_of(far, other):
    return (far % 8) * 2 + other


def kernel(
    x, wall, prev, weights, scale, mean, diag, off,
    moving, shown,
    held, spread, columns, made, spanned, wide, turned, band, state, carried, sums, mixed,
    vweights, vscale, vmean, vdiag, voff,
    in_send, in_recv, halo_send, halo_recv, out_send, out_recv, load_sem, own_sem,
):
    devices = lax.axis_size("span")
    me = lax.axis_index("span")
    base = (me // GROUP) * GROUP
    pos = lax.rem(me, GROUP)
    chip = pos // 2
    core = lax.rem(pos, 2)

    def place(far, other):
        return lax.rem(chip + far + 8, 8) * 2 + lax.rem(core + other, 2)

    before = lax.rem(me + devices - GROUP, devices)
    after = lax.rem(me + GROUP, devices)

    loads = []
    for index, (source, target) in enumerate(
        ((weights, vweights), (scale, vscale), (mean, vmean), (diag, vdiag), (off, voff), (prev, state), (wall, wide))
    ):
        loads.append(pltpu.make_async_copy(source, target, load_sem.at[index]))
        loads[-1].start()
    own = []
    for c in range(3):
        own.append(
            pltpu.make_async_copy(
                x.at[:, c, :, pl.ds(pl.multiple_of(pos * LANES, LANES), LANES)], held.at[c, 8 + pos], own_sem.at[c]
            )
        )
        own[-1].start()

    barrier = pltpu.get_barrier_semaphore()
    for far, other in PEERS:
        pl.semaphore_signal(barrier, inc=1, device_id=(base + place(far, other),), device_id_type=MESH)
    for device in (before, after):
        pl.semaphore_signal(barrier, inc=1, device_id=(device,), device_id_type=MESH)
    pl.semaphore_wait(barrier, len(PEERS) + 2)

    arriving = []
    for c in range(3):
        arriving.append([])
        for far, other in PEERS:
            there = place(far, other)
            slot = slot_of(far, other)
            arriving[c].append(
                pltpu.make_async_remote_copy(
                    src_ref=x.at[:, c, :, pl.ds(pl.multiple_of(there * LANES, LANES), LANES)],
                    dst_ref=held.at[c, 8 + pos],
                    send_sem=in_send.at[c, slot],
                    recv_sem=in_recv.at[c, slot],
                    device_id=(base + there,),
                    device_id_type=MESH,
                )
            )
            arriving[c][-1].start()

    loads[0].wait()
    taps = vweights[...].reshape(1, 2 * HALF + 1)
    taps = (taps / jnp.sqrt(jnp.sum(taps * taps))).astype(jnp.bfloat16).astype(jnp.float32)
    padded = jnp.concatenate([taps, jnp.zeros((1, 1024 - taps.shape[1]), jnp.float32)], axis=1)
    rolled = pltpu.roll(jnp.broadcast_to(padded, (HALF, 1024)), 0, 1, stride=1, stride_axis=0)
    band[...] = rolled[:, : 3 * HALF].astype(jnp.bfloat16)

    loads[6].wait()
    one = (
        lax.broadcasted_iota(jnp.int32, (256, 256), 0) == lax.broadcasted_iota(jnp.int32, (256, 256), 1)
    ).astype(jnp.bfloat16)

    def turn(step, carry):
        row = pl.multiple_of(step * 256, 256)
        for block in range(8):
            piece = wide[pl.ds(row, 256), block * 256 : (block + 1) * 256]
            turned[block * 256 : (block + 1) * 256, pl.ds(row, 256)] = lax.dot_general(
                one, piece, (((1,), (1,)), ((), ())), preferred_element_type=jnp.float32
            ).astype(jnp.bfloat16)
        return carry

    lax.fori_loop(0, 8, turn, 0)

    for index in range(1, 6):
        loads[index].wait()

    flat = held.reshape(3 * 32 * ROWS * 4, LANES)

    def unpack(c, slot):
        first = pl.multiple_of((c * 32 + slot) * LANES, LANES)
        row = pl.multiple_of(slot * LANES, LANES)
        spread[pl.ds(row, LANES), :] = flat[pl.ds(first, LANES), :].astype(jnp.float32)
        for t in range(4):
            columns[pl.ds(pl.multiple_of(slot * ROWS, ROWS), ROWS), t * LANES : (t + 1) * LANES] = spread[
                pl.ds(row + t, ROWS, stride=4), :
            ].astype(jnp.bfloat16)

    halos = []
    leaving = []
    for c in range(3):
        own[c].wait()
        for copy in arriving[c]:
            copy.wait_recv()
        halos.append([])
        for index, (source, target, device) in enumerate(((8, 24, before), (16, 0, after))):
            halos[c].append(
                pltpu.make_async_remote_copy(
                    src_ref=held.at[c, pl.ds(source, 8)],
                    dst_ref=held.at[c, pl.ds(target, 8)],
                    send_sem=halo_send.at[c, index],
                    recv_sem=halo_recv.at[c, index],
                    device_id=(device,),
                    device_id_type=MESH,
                )
            )
            halos[c][-1].start()

        def middle(step, carry):
            for part in range(4):
                unpack(c, 8 + step * 4 + part)
            return carry

        lax.fori_loop(0, 4, middle, 0)
        for copy in halos[c]:
            copy.wait_recv()

        def outer(step, carry):
            for part in range(4):
                unpack(c, step * 4 + part)
                unpack(c, 24 + step * 4 + part)
            return carry

        lax.fori_loop(0, 2, outer, 0)
        for half in range(2):
            block = jnp.dot(
                band[...], columns[half * HALF : half * HALF + 3 * HALF, :], preferred_element_type=jnp.float32
            ).astype(jnp.bfloat16)
            for t in range(4):
                made[c, t, half * HALF : (half + 1) * HALF, :] = block[:, t * LANES : (t + 1) * LANES]
        spanned[c, :, :, pl.ds(pl.multiple_of(pos * LANES, LANES), LANES)] = made[
            c, :, pl.ds(pl.multiple_of(pos * ROWS, ROWS), ROWS), :
        ]
        leaving.append([])
        for far, other in (PEERS if c < 2 else PEERS[::-1]):
            there = place(far, other)
            slot = slot_of(far, other)
            leaving[c].append(
                pltpu.make_async_remote_copy(
                    src_ref=made.at[c, :, pl.ds(pl.multiple_of(there * ROWS, ROWS), ROWS), :],
                    dst_ref=spanned.at[c, :, :, pl.ds(pl.multiple_of(pos * LANES, LANES), LANES)],
                    send_sem=out_send.at[c, slot],
                    recv_sem=out_recv.at[c, slot],
                    device_id=(base + there,),
                    device_id_type=MESH,
                )
            )
            leaving[c][-1].start()

    for c in range(3):
        for index, far in enumerate((0, 1, -1, 2, -2, 3, -3, 4) if c < 2 else (4, -3, 3, -2, 2, -1, 1, 0)):
            for copy, peer in zip(leaving[c], PEERS if c < 2 else PEERS[::-1]):
                if peer[0] == far:
                    copy.wait_recv()
            origin = pl.multiple_of(lax.rem(chip - far + 8, 8) * 256, 256)
            piece = spanned[c, :, :, pl.ds(origin, 256)].reshape(4 * ROWS, 256)
            term = jnp.dot(piece, turned[pl.ds(origin, 256), :], preferred_element_type=jnp.float32)
            if index == 0:
                sums[...] = term
            else:
                sums[...] += term
        for block in range(8):
            cols = slice(block * 256, (block + 1) * 256)
            time = vscale[c : c + 1, cols]
            decay = jnp.exp(-jnp.pi / (2.0 * time))
            inject = jnp.sqrt(1.0 - jnp.exp(-jnp.pi / time))
            value = state[c, :, cols]
            for t in range(4):
                value = decay * value + inject * sums[t * ROWS : (t + 1) * ROWS, cols]
                if c == 0:
                    carried[0, t, :, cols] = value
                    out = vmean[:, cols] + vdiag[0:1, cols] * value
                elif c == 1:
                    along = carried[0, t, :, cols]
                    out = voff[0:1, cols] * along + vdiag[1:2, cols] * value
                    carried[0, t, :, cols] = voff[1:2, cols] * along + voff[2:3, cols] * value
                else:
                    out = carried[0, t, :, cols] + vdiag[2:3, cols] * value
                for side in range(2):
                    mixed[2 * block + side, pl.ds(t, ROWS, stride=4), :] = out[:, side * LANES : (side + 1) * LANES]
            shown[c, :, cols] = value
            for tile in (2 * block, 2 * block + 1):
                moving[c, :, :, tile * LANES : (tile + 1) * LANES] = (
                    mixed[tile].reshape(ROWS, 4, LANES).astype(jnp.bfloat16)
                )

    for c in range(3):
        for copy in arriving[c] + halos[c] + leaving[c]:
            copy.wait_send()


def finish(moving, shown, velocity, final, sems):
    copies = []
    for c in range(3):
        copies.append(pltpu.make_async_copy(moving.at[c], velocity.at[:, c], sems.at[0, c]))
        copies.append(pltpu.make_async_copy(shown.at[c], final.at[c], sems.at[1, c]))
    for copy in copies:
        copy.start()
    for copy in copies:
        copy.wait()


def body(random_slabs, span_weights, wall_filter, prev_state, time_scale, mean_velocity, lund_diag, lund_off):
    rows, planes, parts, width = random_slabs.shape
    any_spec = pl.BlockSpec(memory_space=pl.ANY)
    bf16, f32 = jnp.bfloat16, jnp.float32
    moving, shown = pl.pallas_call(
        kernel,
        out_shape=(
            pltpu.VMEM((parts, rows, planes, width), bf16),
            pltpu.VMEM((parts, rows, width), f32),
        ),
        in_specs=[any_spec] * 8,
        out_specs=(pl.BlockSpec(memory_space=pltpu.VMEM),) * 2,
        scratch_shapes=[
            pltpu.VMEM((3, 32, ROWS, 4, LANES), bf16),
            pltpu.VMEM((4096, LANES), f32),
            pltpu.VMEM((1024, 4 * LANES), bf16),
            pltpu.VMEM((3, 4, 512, LANES), bf16),
            pltpu.VMEM((3, 4, ROWS, width), bf16),
            pltpu.VMEM((width, width), bf16),
            pltpu.VMEM((width, width), bf16),
            pltpu.VMEM((HALF, 3 * HALF), bf16),
            pltpu.VMEM((3, ROWS, width), f32),
            pltpu.VMEM((1, 4, ROWS, width), f32),
            pltpu.VMEM((4 * ROWS, width), f32),
            pltpu.VMEM((width // LANES, 4 * ROWS, LANES), f32),
            pltpu.VMEM((2 * HALF + 1,), f32),
            pltpu.VMEM((3, width), f32),
            pltpu.VMEM((1, width), f32),
            pltpu.VMEM((3, width), f32),
            pltpu.VMEM((3, width), f32),
            pltpu.SemaphoreType.DMA((3, 16)),
            pltpu.SemaphoreType.DMA((3, 16)),
            pltpu.SemaphoreType.DMA((3, 2)),
            pltpu.SemaphoreType.DMA((3, 2)),
            pltpu.SemaphoreType.DMA((3, 16)),
            pltpu.SemaphoreType.DMA((3, 16)),
            pltpu.SemaphoreType.DMA((7,)),
            pltpu.SemaphoreType.DMA((3,)),
        ],
        compiler_params=pltpu.CompilerParams(collective_id=0, has_side_effects=True, vmem_limit_bytes=60 * 2**20),
        name="inflow",
    )(
        random_slabs.transpose(0, 2, 1, 3),
        wall_filter,
        prev_state.transpose(1, 0, 2),
        span_weights,
        time_scale,
        mean_velocity.reshape(1, -1),
        lund_diag,
        lund_off,
    )
    velocity, state = pl.pallas_call(
        finish,
        out_shape=(
            jax.ShapeDtypeStruct((rows, parts, planes, width), bf16),
            jax.ShapeDtypeStruct((parts, rows, width), f32),
        ),
        in_specs=[pl.BlockSpec(memory_space=pltpu.VMEM)] * 2,
        out_specs=(any_spec, any_spec),
        scratch_shapes=[pltpu.SemaphoreType.DMA((2, 3))],
        compiler_params=pltpu.CompilerParams(vmem_limit_bytes=8 * 2**20),
        name="finish",
    )(pltpu.with_memory_space_constraint(moving, pltpu.VMEM), pltpu.with_memory_space_constraint(shown, pltpu.VMEM))
    return velocity.transpose(0, 2, 1, 3), state.transpose(1, 0, 2)


def solution(mesh):
    placed = (P("span", None, None, None), P(), P(), P("span", None, None), P(), P(), P(), P())
    return jax.shard_map(
        body,
        mesh=mesh,
        in_specs=placed,
        out_specs=(P("span", None, None, None), P("span", None, None)),
        check_vma=False,
    )
```

```python
import jax
import jax.numpy as jnp
from jax import lax
from jax.experimental import pallas as pl
from jax.experimental.pallas import tpu as pltpu
from jax.sharding import PartitionSpec as P

MESH = pl.DeviceIdType.MESH
GROUP = 16
ROWS = 32
LANES = 128
HALF = 256
PEERS = [(0, 1)] + [(sign * far, other) for far in (1, 2, 3) for sign in (1, -1) for other in (0, 1)] + [(4, 0), (4, 1)]


NEAR = PEERS[:5]
SCOUT = 8


def wait_for(view, sem):
    pltpu.make_async_copy(view, view, sem).wait()


def kernel(
    x, wall, prev, weights, scale, mean, diag, off,
    moving, shown,
    held, spread, columns, made, spanned, wide, turned, band, state, carried, sums, mixed,
    vweights, vscale, vmean, vdiag, voff,
    in_send, in_recv, halo_send, halo_recv, out_send, out_recv, last_recv, load_sem, chain, scouts, release,
):
    devices = lax.axis_size("span")
    me = lax.axis_index("span")
    base = (me // GROUP) * GROUP
    pos = lax.rem(me, GROUP)
    chip = pos // 2
    core = lax.rem(pos, 2)

    def place(far, other):
        return lax.rem(chip + far + 8, 8) * 2 + lax.rem(core + other, 2)

    before = lax.rem(me + devices - GROUP, devices)
    after = lax.rem(me + GROUP, devices)

    scout = pos == SCOUT
    barrier = pltpu.get_barrier_semaphore()
    for far, other in NEAR:
        pl.semaphore_signal(barrier, inc=1, device_id=(base + place(far, other),), device_id_type=MESH)

    @pl.when(scout)
    def _():
        for device in (before, after):
            pl.semaphore_signal(barrier, inc=1, device_id=(device,), device_id_type=MESH)

    loads = []
    for index, (source, target) in enumerate(
        ((weights, vweights), (scale, vscale), (mean, vmean), (diag, vdiag), (off, voff), (prev, state), (wall, wide))
    ):
        loads.append(pltpu.make_async_copy(source, target, load_sem.at[index]))
        loads[-1].start()
    for c in range(3):
        pltpu.make_async_copy(
            x.at[:, c, :, pl.ds(pl.multiple_of(pos * LANES, LANES), LANES)], held.at[c, 8 + pos], in_recv.at[c]
        ).start()

    def send_in(c, far, other):
        there = place(far, other)
        pltpu.make_async_remote_copy(
            src_ref=x.at[:, c, :, pl.ds(pl.multiple_of(there * LANES, LANES), LANES)],
            dst_ref=held.at[c, 8 + pos],
            send_sem=in_send,
            recv_sem=in_recv.at[c],
            device_id=(base + there,),
            device_id_type=MESH,
        ).start()

    @pl.when(scout)
    def _():
        pl.semaphore_wait(barrier, len(NEAR) + 2)

    @pl.when(jnp.logical_not(scout))
    def _():
        pl.semaphore_wait(barrier, len(NEAR))

    for far, other in NEAR:
        send_in(0, far, other)
    for stage, reach in enumerate(((2, -2), (3, -3), (4,))):

        @pl.when(core == 1)
        def _():
            for sign in (1, -1):
                for other in (0, 1):
                    pl.semaphore_signal(
                        chain.at[stage], inc=1, device_id=(base + place(sign, other),), device_id_type=MESH
                    )

        pl.semaphore_wait(chain.at[stage], 2)
        for far in reach:
            for other in (0, 1):
                send_in(0, far, other)
    for c in (1, 2):
        for far, other in PEERS:
            send_in(c, far, other)

    @pl.when(scout)
    def _():
        for device in (before, after):
            pl.semaphore_signal(scouts, inc=1, device_id=(device,), device_id_type=MESH)

    loads[0].wait()
    taps = vweights[...].reshape(1, 2 * HALF + 1)
    taps = (taps / jnp.sqrt(jnp.sum(taps * taps))).astype(jnp.bfloat16).astype(jnp.float32)
    padded = jnp.concatenate([taps, jnp.zeros((1, 1024 - taps.shape[1]), jnp.float32)], axis=1)
    rolled = pltpu.roll(jnp.broadcast_to(padded, (HALF, 1024)), 0, 1, stride=1, stride_axis=0)
    band[...] = rolled[:, : 3 * HALF].astype(jnp.bfloat16)

    loads[6].wait()
    one = (
        lax.broadcasted_iota(jnp.int32, (256, 256), 0) == lax.broadcasted_iota(jnp.int32, (256, 256), 1)
    ).astype(jnp.bfloat16)

    def turn(step, carry):
        row = pl.multiple_of(step * 256, 256)
        for block in range(8):
            piece = wide[pl.ds(row, 256), block * 256 : (block + 1) * 256]
            turned[block * 256 : (block + 1) * 256, pl.ds(row, 256)] = lax.dot_general(
                one, piece, (((1,), (1,)), ((), ())), preferred_element_type=jnp.float32
            ).astype(jnp.bfloat16)
        return carry

    lax.fori_loop(0, 8, turn, 0)

    for index in range(1, 6):
        loads[index].wait()

    @pl.when(scout)
    def _():
        pl.semaphore_wait(scouts, 2)
        for far, other in PEERS:
            pl.semaphore_signal(release, inc=1, device_id=(base + place(far, other),), device_id_type=MESH)

    @pl.when(jnp.logical_not(scout))
    def _():
        pl.semaphore_wait(release, 1)

    flat = held.reshape(3 * 32 * ROWS * 4, LANES)

    def unpack(c, slot):
        first = pl.multiple_of((c * 32 + slot) * LANES, LANES)
        row = pl.multiple_of(slot * LANES, LANES)
        spread[pl.ds(row, LANES), :] = flat[pl.ds(first, LANES), :].astype(jnp.float32)
        for t in range(4):
            columns[pl.ds(pl.multiple_of(slot * ROWS, ROWS), ROWS), t * LANES : (t + 1) * LANES] = spread[
                pl.ds(row + t, ROWS, stride=4), :
            ].astype(jnp.bfloat16)

    for c in range(3):
        wait_for(held.at[c, pl.ds(8, GROUP)], in_recv.at[c])
        for source, target, device in ((8, 24, before), (16, 0, after)):
            pltpu.make_async_remote_copy(
                src_ref=held.at[c, pl.ds(source, 8)],
                dst_ref=held.at[c, pl.ds(target, 8)],
                send_sem=halo_send,
                recv_sem=halo_recv.at[c],
                device_id=(device,),
                device_id_type=MESH,
            ).start()

        def middle(step, carry):
            for part in range(4):
                unpack(c, 8 + step * 4 + part)
            return carry

        lax.fori_loop(0, 4, middle, 0)
        wait_for(held.at[c, pl.ds(8, GROUP)], halo_recv.at[c])

        def outer(step, carry):
            for part in range(4):
                unpack(c, step * 4 + part)
                unpack(c, 24 + step * 4 + part)
            return carry

        lax.fori_loop(0, 2, outer, 0)
        for half in range(2):
            block = jnp.dot(
                band[...], columns[half * HALF : half * HALF + 3 * HALF, :], preferred_element_type=jnp.float32
            ).astype(jnp.bfloat16)
            for t in range(4):
                made[c, t, half * HALF : (half + 1) * HALF, :] = block[:, t * LANES : (t + 1) * LANES]
        spanned[c, :, :, pl.ds(pl.multiple_of(pos * LANES, LANES), LANES)] = made[
            c, :, pl.ds(pl.multiple_of(pos * ROWS, ROWS), ROWS), :
        ]
        for far, other in PEERS if c < 2 else PEERS[::-1]:
            there = place(far, other)
            pltpu.make_async_remote_copy(
                src_ref=made.at[c, :, pl.ds(pl.multiple_of(there * ROWS, ROWS), ROWS), :],
                dst_ref=spanned.at[c, :, :, pl.ds(pl.multiple_of(pos * LANES, LANES), LANES)],
                send_sem=out_send,
                recv_sem=out_recv.at[c] if c < 2 else last_recv.at[far % 8],
                device_id=(base + there,),
                device_id_type=MESH,
            ).start()

    for c in range(3):
        if c < 2:
            wait_for(spanned.at[c, :, :, pl.ds(0, 15 * LANES)], out_recv.at[c])
        for index, far in enumerate((4, -3, 3, -2, 2, -1, 1, 0)):
            if c == 2:
                wait_for(spanned.at[c, :, :, pl.ds(0, 2 * LANES if far else LANES)], last_recv.at[far % 8])
            origin = pl.multiple_of(lax.rem(chip - far + 8, 8) * 256, 256)
            piece = spanned[c, :, :, pl.ds(origin, 256)].reshape(4 * ROWS, 256)
            term = jnp.dot(piece, turned[pl.ds(origin, 256), :], preferred_element_type=jnp.float32)
            if index == 0:
                sums[...] = term
            else:
                sums[...] += term
        for block in range(8):
            cols = slice(block * 256, (block + 1) * 256)
            time = vscale[c : c + 1, cols]
            decay = jnp.exp(-jnp.pi / (2.0 * time))
            inject = jnp.sqrt(1.0 - jnp.exp(-jnp.pi / time))
            value = state[c, :, cols]
            for t in range(4):
                value = decay * value + inject * sums[t * ROWS : (t + 1) * ROWS, cols]
                if c == 0:
                    carried[0, t, :, cols] = value
                    out = vmean[:, cols] + vdiag[0:1, cols] * value
                elif c == 1:
                    along = carried[0, t, :, cols]
                    out = voff[0:1, cols] * along + vdiag[1:2, cols] * value
                    carried[0, t, :, cols] = voff[1:2, cols] * along + voff[2:3, cols] * value
                else:
                    out = carried[0, t, :, cols] + vdiag[2:3, cols] * value
                for side in range(2):
                    mixed[2 * block + side, pl.ds(t, ROWS, stride=4), :] = out[:, side * LANES : (side + 1) * LANES]
            shown[c, :, cols] = value
            for tile in (2 * block, 2 * block + 1):
                moving[c, :, :, tile * LANES : (tile + 1) * LANES] = (
                    mixed[tile].reshape(ROWS, 4, LANES).astype(jnp.bfloat16)
                )

    wait_for(x.at[:, :, :, pl.ds(0, 15 * LANES)], in_send)
    wait_for(held.at[:, pl.ds(0, GROUP)], halo_send)
    wait_for(made.at[:, :, pl.ds(0, 15 * ROWS), :], out_send)


def finish(moving, shown, velocity, final, sems):
    copies = []
    for c in range(3):
        copies.append(pltpu.make_async_copy(moving.at[c], velocity.at[:, c], sems.at[0, c]))
        copies.append(pltpu.make_async_copy(shown.at[c], final.at[c], sems.at[1, c]))
    for copy in copies:
        copy.start()
    for copy in copies:
        copy.wait()


def body(random_slabs, span_weights, wall_filter, prev_state, time_scale, mean_velocity, lund_diag, lund_off):
    rows, planes, parts, width = random_slabs.shape
    any_spec = pl.BlockSpec(memory_space=pl.ANY)
    bf16, f32 = jnp.bfloat16, jnp.float32
    moving, shown = pl.pallas_call(
        kernel,
        out_shape=(
            pltpu.VMEM((parts, rows, planes, width), bf16),
            pltpu.VMEM((parts, rows, width), f32),
        ),
        in_specs=[any_spec] * 8,
        out_specs=(pl.BlockSpec(memory_space=pltpu.VMEM),) * 2,
        scratch_shapes=[
            pltpu.VMEM((3, 32, ROWS, 4, LANES), bf16),
            pltpu.VMEM((4096, LANES), f32),
            pltpu.VMEM((1024, 4 * LANES), bf16),
            pltpu.VMEM((3, 4, 512, LANES), bf16),
            pltpu.VMEM((3, 4, ROWS, width), bf16),
            pltpu.VMEM((width, width), bf16),
            pltpu.VMEM((width, width), bf16),
            pltpu.VMEM((HALF, 3 * HALF), bf16),
            pltpu.VMEM((3, ROWS, width), f32),
            pltpu.VMEM((1, 4, ROWS, width), f32),
            pltpu.VMEM((4 * ROWS, width), f32),
            pltpu.VMEM((width // LANES, 4 * ROWS, LANES), f32),
            pltpu.VMEM((2 * HALF + 1,), f32),
            pltpu.VMEM((3, width), f32),
            pltpu.VMEM((1, width), f32),
            pltpu.VMEM((3, width), f32),
            pltpu.VMEM((3, width), f32),
            pltpu.SemaphoreType.DMA,
            pltpu.SemaphoreType.DMA((3,)),
            pltpu.SemaphoreType.DMA,
            pltpu.SemaphoreType.DMA((3,)),
            pltpu.SemaphoreType.DMA,
            pltpu.SemaphoreType.DMA((2,)),
            pltpu.SemaphoreType.DMA((8,)),
            pltpu.SemaphoreType.DMA((7,)),
            pltpu.SemaphoreType.REGULAR((3,)),
            pltpu.SemaphoreType.REGULAR,
            pltpu.SemaphoreType.REGULAR,
        ],
        compiler_params=pltpu.CompilerParams(collective_id=0, has_side_effects=True, vmem_limit_bytes=60 * 2**20),
        name="inflow",
    )(
        random_slabs.transpose(0, 2, 1, 3),
        wall_filter,
        prev_state.transpose(1, 0, 2),
        span_weights,
        time_scale,
        mean_velocity.reshape(1, -1),
        lund_diag,
        lund_off,
    )
    velocity, state = pl.pallas_call(
        finish,
        out_shape=(
            jax.ShapeDtypeStruct((rows, parts, planes, width), bf16),
            jax.ShapeDtypeStruct((parts, rows, width), f32),
        ),
        in_specs=[pl.BlockSpec(memory_space=pltpu.VMEM)] * 2,
        out_specs=(any_spec, any_spec),
        scratch_shapes=[pltpu.SemaphoreType.DMA((2, 3))],
        compiler_params=pltpu.CompilerParams(vmem_limit_bytes=8 * 2**20),
        name="finish",
    )(pltpu.with_memory_space_constraint(moving, pltpu.VMEM), pltpu.with_memory_space_constraint(shown, pltpu.VMEM))
    return velocity.transpose(0, 2, 1, 3), state.transpose(1, 0, 2)


def solution(mesh):
    placed = (P("span", None, None, None), P(), P(), P("span", None, None), P(), P(), P(), P())
    return jax.shard_map(
        body,
        mesh=mesh,
        in_specs=placed,
        out_specs=(P("span", None, None, None), P("span", None, None)),
        check_vma=False,
    )
```

```python
import jax
import jax.numpy as jnp
from jax import lax
from jax.experimental import pallas as pl
from jax.experimental.pallas import tpu as pltpu
from jax.sharding import PartitionSpec as P

MESH = pl.DeviceIdType.MESH
GROUP = 16
ROWS = 32
LANES = 128
HALF = 256
PEERS = [(0, 1)] + [(sign * far, other) for far in (1, 2, 3) for sign in (1, -1) for other in (0, 1)] + [(4, 0), (4, 1)]


FARS = (1, -1, 2, -2, 3, -3, 4)
ORDER = (0, 1, 2, 3, 7, 4, 6, 5)
SCOUT = 0


def rank(chip):
    return jnp.minimum(2 * chip, 22 - 2 * chip) + jnp.where(chip == 5, 1, 0)


def wait_for(view, sem):
    pltpu.make_async_copy(view, view, sem).wait()


def kernel(
    x, wall, prev, weights, scale, mean, diag, off,
    moving, shown,
    held, spread, columns, made, spanned, wide, turned, band, state, carried, sums, mixed,
    vweights, vscale, vmean, vdiag, voff,
    in_send, in_recv, halo_send, halo_recv, out_send, out_recv, last_recv, load_sem, ready, scouts, release,
):
    devices = lax.axis_size("span")
    me = lax.axis_index("span")
    base = (me // GROUP) * GROUP
    pos = lax.rem(me, GROUP)
    chip = pos // 2
    core = lax.rem(pos, 2)

    def place(far, other):
        return lax.rem(chip + far + 8, 8) * 2 + lax.rem(core + other, 2)

    before = lax.rem(me + devices - GROUP, devices)
    after = lax.rem(me + GROUP, devices)

    scout = pos == SCOUT
    barrier = pltpu.get_barrier_semaphore()
    mine = rank(chip)
    ranks = {far: rank(lax.rem(chip + far + 8, 8)) for far in FARS}

    def signal_chip(far, sem):
        for other in (0, 1):
            pl.semaphore_signal(sem, inc=1, device_id=(base + place(far, other),), device_id_type=MESH)

    pl.semaphore_signal(barrier, inc=1, device_id=(base + place(0, 1),), device_id_type=MESH)
    for far in FARS:

        @pl.when(ranks[far] > mine)
        def _():
            signal_chip(far, barrier)

    @pl.when(scout)
    def _():
        for device in (before, after):
            pl.semaphore_signal(barrier, inc=1, device_id=(device,), device_id_type=MESH)

    loads = []
    for index, (source, target) in enumerate(
        ((weights, vweights), (scale, vscale), (mean, vmean), (diag, vdiag), (off, voff), (prev, state), (wall, wide))
    ):
        loads.append(pltpu.make_async_copy(source, target, load_sem.at[index]))
        loads[-1].start()
    for c in range(3):
        pltpu.make_async_copy(
            x.at[:, c, :, pl.ds(pl.multiple_of(pos * LANES, LANES), LANES)], held.at[c, 8 + pos], in_recv.at[c]
        ).start()

    def send_in(c, far, other):
        there = place(far, other)
        pltpu.make_async_remote_copy(
            src_ref=x.at[:, c, :, pl.ds(pl.multiple_of(there * LANES, LANES), LANES)],
            dst_ref=held.at[c, 8 + pos],
            send_sem=in_send,
            recv_sem=in_recv.at[c],
            device_id=(base + there,),
            device_id_type=MESH,
        ).start()

    for level, greeted in ((0, 0), (2, 1), (4, 2), (6, 3), (8, 4), (10, 6), (11, 7)):

        @pl.when(mine == level)
        def _():
            if level == 0:

                @pl.when(scout)
                def _():
                    pl.semaphore_wait(barrier, 3)

                @pl.when(jnp.logical_not(scout))
                def _():
                    pl.semaphore_wait(barrier, 1)

            else:
                pl.semaphore_wait(barrier, 2 * greeted + 1)

    for far in FARS:

        @pl.when(ranks[far] < mine)
        def _():
            signal_chip(far, ready.at[chip])

    send_in(0, 0, 1)
    for far in FARS:

        @pl.when(ranks[far] > mine)
        def _():
            pl.semaphore_wait(ready.at[lax.rem(chip + far + 8, 8)], 2)

        for other in (0, 1):
            send_in(0, far, other)
    for c in (1, 2):
        for far, other in PEERS:
            send_in(c, far, other)

    @pl.when(scout)
    def _():
        for device in (before, after):
            pl.semaphore_signal(scouts, inc=1, device_id=(device,), device_id_type=MESH)

    loads[0].wait()
    taps = vweights[...].reshape(1, 2 * HALF + 1)
    taps = (taps / jnp.sqrt(jnp.sum(taps * taps))).astype(jnp.bfloat16).astype(jnp.float32)
    padded = jnp.concatenate([taps, jnp.zeros((1, 1024 - taps.shape[1]), jnp.float32)], axis=1)
    rolled = pltpu.roll(jnp.broadcast_to(padded, (HALF, 1024)), 0, 1, stride=1, stride_axis=0)
    band[...] = rolled[:, : 3 * HALF].astype(jnp.bfloat16)

    loads[6].wait()
    one = (
        lax.broadcasted_iota(jnp.int32, (256, 256), 0) == lax.broadcasted_iota(jnp.int32, (256, 256), 1)
    ).astype(jnp.bfloat16)

    def turn(step, carry):
        row = pl.multiple_of(step * 256, 256)
        for block in range(8):
            piece = wide[pl.ds(row, 256), block * 256 : (block + 1) * 256]
            turned[block * 256 : (block + 1) * 256, pl.ds(row, 256)] = lax.dot_general(
                one, piece, (((1,), (1,)), ((), ())), preferred_element_type=jnp.float32
            ).astype(jnp.bfloat16)
        return carry

    lax.fori_loop(0, 8, turn, 0)

    for index in range(1, 6):
        loads[index].wait()

    @pl.when(scout)
    def _():
        pl.semaphore_wait(scouts, 2)
        for far, other in PEERS:
            pl.semaphore_signal(release, inc=1, device_id=(base + place(far, other),), device_id_type=MESH)

    @pl.when(jnp.logical_not(scout))
    def _():
        pl.semaphore_wait(release, 1)

    flat = held.reshape(3 * 32 * ROWS * 4, LANES)

    def unpack(c, slot):
        first = pl.multiple_of((c * 32 + slot) * LANES, LANES)
        row = pl.multiple_of(slot * LANES, LANES)
        spread[pl.ds(row, LANES), :] = flat[pl.ds(first, LANES), :].astype(jnp.float32)
        for t in range(4):
            columns[pl.ds(pl.multiple_of(slot * ROWS, ROWS), ROWS), t * LANES : (t + 1) * LANES] = spread[
                pl.ds(row + t, ROWS, stride=4), :
            ].astype(jnp.bfloat16)

    for c in range(3):
        wait_for(held.at[c, pl.ds(8, GROUP)], in_recv.at[c])
        for source, target, device in ((8, 24, before), (16, 0, after)):
            pltpu.make_async_remote_copy(
                src_ref=held.at[c, pl.ds(source, 8)],
                dst_ref=held.at[c, pl.ds(target, 8)],
                send_sem=halo_send,
                recv_sem=halo_recv.at[c],
                device_id=(device,),
                device_id_type=MESH,
            ).start()

        def middle(step, carry):
            for part in range(4):
                unpack(c, 8 + step * 4 + part)
            return carry

        lax.fori_loop(0, 4, middle, 0)
        wait_for(held.at[c, pl.ds(8, GROUP)], halo_recv.at[c])

        def outer(step, carry):
            for part in range(4):
                unpack(c, step * 4 + part)
                unpack(c, 24 + step * 4 + part)
            return carry

        lax.fori_loop(0, 2, outer, 0)
        for half in range(2):
            block = jnp.dot(
                band[...], columns[half * HALF : half * HALF + 3 * HALF, :], preferred_element_type=jnp.float32
            ).astype(jnp.bfloat16)
            for t in range(4):
                made[c, t, half * HALF : (half + 1) * HALF, :] = block[:, t * LANES : (t + 1) * LANES]
        spanned[c, :, :, pl.ds(pl.multiple_of(pos * LANES, LANES), LANES)] = made[
            c, :, pl.ds(pl.multiple_of(pos * ROWS, ROWS), ROWS), :
        ]
        def send_out(there, sem):
            pltpu.make_async_remote_copy(
                src_ref=made.at[c, :, pl.ds(pl.multiple_of(there * ROWS, ROWS), ROWS), :],
                dst_ref=spanned.at[c, :, :, pl.ds(pl.multiple_of(pos * LANES, LANES), LANES)],
                send_sem=out_send,
                recv_sem=sem,
                device_id=(base + there,),
                device_id_type=MESH,
            ).start()

        if c < 2:
            for far, other in PEERS:
                send_out(place(far, other), out_recv.at[c])
        else:
            for target in ORDER:
                for side in (0, 1):

                    @pl.when(pos != 2 * target + side)
                    def _():
                        send_out(2 * target + side, last_recv.at[lax.rem(target - chip + 8, 8)])

    for c in range(3):
        if c < 2:
            wait_for(spanned.at[c, :, :, pl.ds(0, 15 * LANES)], out_recv.at[c])
        for index, far in enumerate((0, 1, -1, 2, -2, 3, -3, 4)):
            if c == 2:
                wait_for(spanned.at[c, :, :, pl.ds(0, 2 * LANES if far else LANES)], last_recv.at[far % 8])
            origin = pl.multiple_of(lax.rem(chip - far + 8, 8) * 256, 256)
            piece = spanned[c, :, :, pl.ds(origin, 256)].reshape(4 * ROWS, 256)
            term = jnp.dot(piece, turned[pl.ds(origin, 256), :], preferred_element_type=jnp.float32)
            if index == 0:
                sums[...] = term
            else:
                sums[...] += term
        for block in range(8):
            cols = slice(block * 256, (block + 1) * 256)
            time = vscale[c : c + 1, cols]
            decay = jnp.exp(-jnp.pi / (2.0 * time))
            inject = jnp.sqrt(1.0 - jnp.exp(-jnp.pi / time))
            value = state[c, :, cols]
            for t in range(4):
                value = decay * value + inject * sums[t * ROWS : (t + 1) * ROWS, cols]
                if c == 0:
                    carried[0, t, :, cols] = value
                    out = vmean[:, cols] + vdiag[0:1, cols] * value
                elif c == 1:
                    along = carried[0, t, :, cols]
                    out = voff[0:1, cols] * along + vdiag[1:2, cols] * value
                    carried[0, t, :, cols] = voff[1:2, cols] * along + voff[2:3, cols] * value
                else:
                    out = carried[0, t, :, cols] + vdiag[2:3, cols] * value
                for side in range(2):
                    mixed[2 * block + side, pl.ds(t, ROWS, stride=4), :] = out[:, side * LANES : (side + 1) * LANES]
            shown[c, :, cols] = value
            for tile in (2 * block, 2 * block + 1):
                moving[c, :, :, tile * LANES : (tile + 1) * LANES] = (
                    mixed[tile].reshape(ROWS, 4, LANES).astype(jnp.bfloat16)
                )

    wait_for(x.at[:, :, :, pl.ds(0, 15 * LANES)], in_send)
    wait_for(held.at[:, pl.ds(0, GROUP)], halo_send)
    wait_for(made.at[:, :, pl.ds(0, 15 * ROWS), :], out_send)


def finish(moving, shown, velocity, final, sems):
    copies = []
    for c in range(3):
        copies.append(pltpu.make_async_copy(moving.at[c], velocity.at[:, c], sems.at[0, c]))
        copies.append(pltpu.make_async_copy(shown.at[c], final.at[c], sems.at[1, c]))
    for copy in copies:
        copy.start()
    for copy in copies:
        copy.wait()


def body(random_slabs, span_weights, wall_filter, prev_state, time_scale, mean_velocity, lund_diag, lund_off):
    rows, planes, parts, width = random_slabs.shape
    any_spec = pl.BlockSpec(memory_space=pl.ANY)
    bf16, f32 = jnp.bfloat16, jnp.float32
    moving, shown = pl.pallas_call(
        kernel,
        out_shape=(
            pltpu.VMEM((parts, rows, planes, width), bf16),
            pltpu.VMEM((parts, rows, width), f32),
        ),
        in_specs=[any_spec] * 8,
        out_specs=(pl.BlockSpec(memory_space=pltpu.VMEM),) * 2,
        scratch_shapes=[
            pltpu.VMEM((3, 32, ROWS, 4, LANES), bf16),
            pltpu.VMEM((4096, LANES), f32),
            pltpu.VMEM((1024, 4 * LANES), bf16),
            pltpu.VMEM((3, 4, 512, LANES), bf16),
            pltpu.VMEM((3, 4, ROWS, width), bf16),
            pltpu.VMEM((width, width), bf16),
            pltpu.VMEM((width, width), bf16),
            pltpu.VMEM((HALF, 3 * HALF), bf16),
            pltpu.VMEM((3, ROWS, width), f32),
            pltpu.VMEM((1, 4, ROWS, width), f32),
            pltpu.VMEM((4 * ROWS, width), f32),
            pltpu.VMEM((width // LANES, 4 * ROWS, LANES), f32),
            pltpu.VMEM((2 * HALF + 1,), f32),
            pltpu.VMEM((3, width), f32),
            pltpu.VMEM((1, width), f32),
            pltpu.VMEM((3, width), f32),
            pltpu.VMEM((3, width), f32),
            pltpu.SemaphoreType.DMA,
            pltpu.SemaphoreType.DMA((3,)),
            pltpu.SemaphoreType.DMA,
            pltpu.SemaphoreType.DMA((3,)),
            pltpu.SemaphoreType.DMA,
            pltpu.SemaphoreType.DMA((2,)),
            pltpu.SemaphoreType.DMA((8,)),
            pltpu.SemaphoreType.DMA((7,)),
            pltpu.SemaphoreType.REGULAR((8,)),
            pltpu.SemaphoreType.REGULAR,
            pltpu.SemaphoreType.REGULAR,
        ],
        compiler_params=pltpu.CompilerParams(collective_id=0, has_side_effects=True, vmem_limit_bytes=60 * 2**20),
        name="inflow",
    )(
        random_slabs.transpose(0, 2, 1, 3),
        wall_filter,
        prev_state.transpose(1, 0, 2),
        span_weights,
        time_scale,
        mean_velocity.reshape(1, -1),
        lund_diag,
        lund_off,
    )
    velocity, state = pl.pallas_call(
        finish,
        out_shape=(
            jax.ShapeDtypeStruct((rows, parts, planes, width), bf16),
            jax.ShapeDtypeStruct((parts, rows, width), f32),
        ),
        in_specs=[pl.BlockSpec(memory_space=pltpu.VMEM)] * 2,
        out_specs=(any_spec, any_spec),
        scratch_shapes=[pltpu.SemaphoreType.DMA((2, 3))],
        compiler_params=pltpu.CompilerParams(vmem_limit_bytes=8 * 2**20),
        name="finish",
    )(pltpu.with_memory_space_constraint(moving, pltpu.VMEM), pltpu.with_memory_space_constraint(shown, pltpu.VMEM))
    return velocity.transpose(0, 2, 1, 3), state.transpose(1, 0, 2)


def solution(mesh):
    placed = (P("span", None, None, None), P(), P(), P("span", None, None), P(), P(), P(), P())
    return jax.shard_map(
        body,
        mesh=mesh,
        in_specs=placed,
        out_specs=(P("span", None, None, None), P("span", None, None)),
        check_vma=False,
    )
```

```python
import jax
import jax.numpy as jnp
from jax import lax
from jax.experimental import pallas as pl
from jax.experimental.pallas import tpu as pltpu
from jax.sharding import PartitionSpec as P

MESH = pl.DeviceIdType.MESH
GROUP = 16
ROWS = 32
LANES = 128
HALF = 256
PEERS = [(0, 1)] + [(sign * far, other) for far in (1, 2, 3) for sign in (1, -1) for other in (0, 1)] + [(4, 0), (4, 1)]


ORDER = (0, 1, 2, 3, 7, 4, 6, 5)
SCOUT = 0


EARLIER = {0: (), 1: (0,), 2: (0, 1), 3: (0, 1, 2), 4: (0, 1, 2, 3), 5: (0, 1, 2, 3, 4), 6: (0, 1, 4, 7), 7: (0, 1)}
RELAY = 8
ENTRY = {
    0: (("wait", 1), 1, ("wait", 2), 2, ("wait", 7), 7, ("wait", 3), 3, ("wait", 6), 6, ("wait", 4), 4, ("wait", 5), 5),
    1: (0, ("wait", 2), 2, ("wait", 3), 3, ("wait", 7), 7, ("wait", 4), 4, ("wait", 6), 6, ("wait", 5), 5),
    2: (1, 0, ("wait", 3), 3, ("wait", 4), 4, ("wait", 5), 5, ("wait", RELAY), 6, 7),
    3: (2, 1, 0, ("wait", 4), 4, ("wait", 5), 5, ("wait", RELAY), 6, 7),
    4: (3, 2, 1, 0, ("wait", 5), ("wait", 6), ("relay", (5, 6, 3, 2)), 5, 6, 7),
    5: (4, 3, 2, 1, 0, ("wait", RELAY), 6, 7),
    6: (7, 4, 0, 1, ("wait", RELAY), ("relay", (7,)), 5, 2, 3),
    7: (0, 1, ("wait", 6), 6, 4, ("wait", RELAY), 5, 2, 3),
}


def wait_for(view, sem):
    pltpu.make_async_copy(view, view, sem).wait()


def kernel(
    x, wall, prev, weights, scale, mean, diag, off,
    moving, shown,
    held, spread, columns, made, spanned, wide, turned, band, state, carried, sums, mixed,
    vweights, vscale, vmean, vdiag, voff,
    in_send, in_recv, halo_send, halo_recv, out_send, out_recv, last_recv, load_sem, ready, scouts, release,
):
    devices = lax.axis_size("span")
    me = lax.axis_index("span")
    base = (me // GROUP) * GROUP
    pos = lax.rem(me, GROUP)
    chip = pos // 2
    core = lax.rem(pos, 2)

    def place(far, other):
        return lax.rem(chip + far + 8, 8) * 2 + lax.rem(core + other, 2)

    before = lax.rem(me + devices - GROUP, devices)
    after = lax.rem(me + GROUP, devices)

    scout = pos == SCOUT
    barrier = pltpu.get_barrier_semaphore()

    def signal_chip(target, sem):
        for side in (0, 1):
            pl.semaphore_signal(sem, inc=1, device_id=(base + 2 * target + side,), device_id_type=MESH)

    pl.semaphore_signal(barrier, inc=1, device_id=(base + place(0, 1),), device_id_type=MESH)
    for which in range(8):

        @pl.when(chip == which)
        def _():
            for target in ORDER:
                if which in EARLIER[target]:
                    signal_chip(target, barrier)

    @pl.when(scout)
    def _():
        for device in (before, after):
            pl.semaphore_signal(barrier, inc=1, device_id=(device,), device_id_type=MESH)

    loads = []
    for index, (source, target) in enumerate(
        ((weights, vweights), (scale, vscale), (mean, vmean), (diag, vdiag), (off, voff), (prev, state), (wall, wide))
    ):
        loads.append(pltpu.make_async_copy(source, target, load_sem.at[index]))
        loads[-1].start()
    for c in range(3):
        pltpu.make_async_copy(
            x.at[:, c, :, pl.ds(pl.multiple_of(pos * LANES, LANES), LANES)], held.at[c, 8 + pos], in_recv.at[c]
        ).start()

    def send_in(c, there):
        pltpu.make_async_remote_copy(
            src_ref=x.at[:, c, :, pl.ds(pl.multiple_of(there * LANES, LANES), LANES)],
            dst_ref=held.at[c, 8 + pos],
            send_sem=in_send,
            recv_sem=in_recv.at[c],
            device_id=(base + there,),
            device_id_type=MESH,
        ).start()

    @pl.when(scout)
    def _():
        pl.semaphore_wait(barrier, 3)

    for which in range(8):

        @pl.when(jnp.logical_and(chip == which, jnp.logical_not(scout)))
        def _():
            pl.semaphore_wait(barrier, 2 * len(EARLIER[which]) + 1)

        @pl.when(chip == which)
        def _():
            for target in EARLIER[which]:
                signal_chip(target, ready.at[which])
            send_in(0, place(0, 1))
            for step in ENTRY[which]:
                if isinstance(step, int):
                    send_in(0, 2 * step)
                    send_in(0, 2 * step + 1)
                elif step[0] == "wait":
                    pl.semaphore_wait(ready.at[step[1]], 2)
                else:
                    for target in step[1]:
                        signal_chip(target, ready.at[RELAY])

    for c in (1, 2):
        for far, other in PEERS:
            send_in(c, place(far, other))

    @pl.when(scout)
    def _():
        for device in (before, after):
            pl.semaphore_signal(scouts, inc=1, device_id=(device,), device_id_type=MESH)

    loads[0].wait()
    taps = vweights[...].reshape(1, 2 * HALF + 1)
    taps = (taps / jnp.sqrt(jnp.sum(taps * taps))).astype(jnp.bfloat16).astype(jnp.float32)
    padded = jnp.concatenate([taps, jnp.zeros((1, 1024 - taps.shape[1]), jnp.float32)], axis=1)
    rolled = pltpu.roll(jnp.broadcast_to(padded, (HALF, 1024)), 0, 1, stride=1, stride_axis=0)
    band[...] = rolled[:, : 3 * HALF].astype(jnp.bfloat16)

    loads[6].wait()
    one = (
        lax.broadcasted_iota(jnp.int32, (256, 256), 0) == lax.broadcasted_iota(jnp.int32, (256, 256), 1)
    ).astype(jnp.bfloat16)

    def turn(step, carry):
        row = pl.multiple_of(step * 256, 256)
        for block in range(8):
            piece = wide[pl.ds(row, 256), block * 256 : (block + 1) * 256]
            turned[block * 256 : (block + 1) * 256, pl.ds(row, 256)] = lax.dot_general(
                one, piece, (((1,), (1,)), ((), ())), preferred_element_type=jnp.float32
            ).astype(jnp.bfloat16)
        return carry

    lax.fori_loop(0, 8, turn, 0)

    for index in range(1, 6):
        loads[index].wait()

    @pl.when(scout)
    def _():
        pl.semaphore_wait(scouts, 2)
        for far, other in PEERS:
            pl.semaphore_signal(release, inc=1, device_id=(base + place(far, other),), device_id_type=MESH)

    @pl.when(jnp.logical_not(scout))
    def _():
        pl.semaphore_wait(release, 1)

    flat = held.reshape(3 * 32 * ROWS * 4, LANES)

    def unpack(c, slot):
        first = pl.multiple_of((c * 32 + slot) * LANES, LANES)
        row = pl.multiple_of(slot * LANES, LANES)
        spread[pl.ds(row, LANES), :] = flat[pl.ds(first, LANES), :].astype(jnp.float32)
        for t in range(4):
            columns[pl.ds(pl.multiple_of(slot * ROWS, ROWS), ROWS), t * LANES : (t + 1) * LANES] = spread[
                pl.ds(row + t, ROWS, stride=4), :
            ].astype(jnp.bfloat16)

    for c in range(3):
        wait_for(held.at[c, pl.ds(8, GROUP)], in_recv.at[c])
        for source, target, device in ((8, 24, before), (16, 0, after)):
            pltpu.make_async_remote_copy(
                src_ref=held.at[c, pl.ds(source, 8)],
                dst_ref=held.at[c, pl.ds(target, 8)],
                send_sem=halo_send,
                recv_sem=halo_recv.at[c],
                device_id=(device,),
                device_id_type=MESH,
            ).start()

        def middle(step, carry):
            for part in range(4):
                unpack(c, 8 + step * 4 + part)
            return carry

        lax.fori_loop(0, 4, middle, 0)
        wait_for(held.at[c, pl.ds(8, GROUP)], halo_recv.at[c])

        def outer(step, carry):
            for part in range(4):
                unpack(c, step * 4 + part)
                unpack(c, 24 + step * 4 + part)
            return carry

        lax.fori_loop(0, 2, outer, 0)
        for half in range(2):
            block = jnp.dot(
                band[...], columns[half * HALF : half * HALF + 3 * HALF, :], preferred_element_type=jnp.float32
            ).astype(jnp.bfloat16)
            for t in range(4):
                made[c, t, half * HALF : (half + 1) * HALF, :] = block[:, t * LANES : (t + 1) * LANES]
        spanned[c, :, :, pl.ds(pl.multiple_of(pos * LANES, LANES), LANES)] = made[
            c, :, pl.ds(pl.multiple_of(pos * ROWS, ROWS), ROWS), :
        ]
        def send_out(there, sem):
            pltpu.make_async_remote_copy(
                src_ref=made.at[c, :, pl.ds(pl.multiple_of(there * ROWS, ROWS), ROWS), :],
                dst_ref=spanned.at[c, :, :, pl.ds(pl.multiple_of(pos * LANES, LANES), LANES)],
                send_sem=out_send,
                recv_sem=sem,
                device_id=(base + there,),
                device_id_type=MESH,
            ).start()

        if c < 2:
            for far, other in PEERS:
                send_out(place(far, other), out_recv.at[c])
        else:
            for target in ORDER:
                for side in (0, 1):

                    @pl.when(pos != 2 * target + side)
                    def _():
                        send_out(2 * target + side, last_recv.at[lax.rem(target - chip + 8, 8)])

    for c in range(3):
        if c < 2:
            wait_for(spanned.at[c, :, :, pl.ds(0, 15 * LANES)], out_recv.at[c])
        for index, far in enumerate((0, 1, -1, 2, -2, 3, -3, 4)):
            if c == 2:
                wait_for(spanned.at[c, :, :, pl.ds(0, 2 * LANES if far else LANES)], last_recv.at[far % 8])
            origin = pl.multiple_of(lax.rem(chip - far + 8, 8) * 256, 256)
            piece = spanned[c, :, :, pl.ds(origin, 256)].reshape(4 * ROWS, 256)
            term = jnp.dot(piece, turned[pl.ds(origin, 256), :], preferred_element_type=jnp.float32)
            if index == 0:
                sums[...] = term
            else:
                sums[...] += term
        for block in range(8):
            cols = slice(block * 256, (block + 1) * 256)
            time = vscale[c : c + 1, cols]
            decay = jnp.exp(-jnp.pi / (2.0 * time))
            inject = jnp.sqrt(1.0 - jnp.exp(-jnp.pi / time))
            value = state[c, :, cols]
            for t in range(4):
                value = decay * value + inject * sums[t * ROWS : (t + 1) * ROWS, cols]
                if c == 0:
                    carried[0, t, :, cols] = value
                    out = vmean[:, cols] + vdiag[0:1, cols] * value
                elif c == 1:
                    along = carried[0, t, :, cols]
                    out = voff[0:1, cols] * along + vdiag[1:2, cols] * value
                    carried[0, t, :, cols] = voff[1:2, cols] * along + voff[2:3, cols] * value
                else:
                    out = carried[0, t, :, cols] + vdiag[2:3, cols] * value
                for side in range(2):
                    mixed[2 * block + side, pl.ds(t, ROWS, stride=4), :] = out[:, side * LANES : (side + 1) * LANES]
            shown[c, :, cols] = value
            for tile in (2 * block, 2 * block + 1):
                moving[c, :, :, tile * LANES : (tile + 1) * LANES] = (
                    mixed[tile].reshape(ROWS, 4, LANES).astype(jnp.bfloat16)
                )

    wait_for(x.at[:, :, :, pl.ds(0, 15 * LANES)], in_send)
    wait_for(held.at[:, pl.ds(0, GROUP)], halo_send)
    wait_for(made.at[:, :, pl.ds(0, 15 * ROWS), :], out_send)


def finish(moving, shown, velocity, final, sems):
    copies = []
    for c in range(3):
        copies.append(pltpu.make_async_copy(moving.at[c], velocity.at[:, c], sems.at[0, c]))
        copies.append(pltpu.make_async_copy(shown.at[c], final.at[c], sems.at[1, c]))
    for copy in copies:
        copy.start()
    for copy in copies:
        copy.wait()


def body(random_slabs, span_weights, wall_filter, prev_state, time_scale, mean_velocity, lund_diag, lund_off):
    rows, planes, parts, width = random_slabs.shape
    any_spec = pl.BlockSpec(memory_space=pl.ANY)
    bf16, f32 = jnp.bfloat16, jnp.float32
    moving, shown = pl.pallas_call(
        kernel,
        out_shape=(
            pltpu.VMEM((parts, rows, planes, width), bf16),
            pltpu.VMEM((parts, rows, width), f32),
        ),
        in_specs=[any_spec] * 8,
        out_specs=(pl.BlockSpec(memory_space=pltpu.VMEM),) * 2,
        scratch_shapes=[
            pltpu.VMEM((3, 32, ROWS, 4, LANES), bf16),
            pltpu.VMEM((4096, LANES), f32),
            pltpu.VMEM((1024, 4 * LANES), bf16),
            pltpu.VMEM((3, 4, 512, LANES), bf16),
            pltpu.VMEM((3, 4, ROWS, width), bf16),
            pltpu.VMEM((width, width), bf16),
            pltpu.VMEM((width, width), bf16),
            pltpu.VMEM((HALF, 3 * HALF), bf16),
            pltpu.VMEM((3, ROWS, width), f32),
            pltpu.VMEM((1, 4, ROWS, width), f32),
            pltpu.VMEM((4 * ROWS, width), f32),
            pltpu.VMEM((width // LANES, 4 * ROWS, LANES), f32),
            pltpu.VMEM((2 * HALF + 1,), f32),
            pltpu.VMEM((3, width), f32),
            pltpu.VMEM((1, width), f32),
            pltpu.VMEM((3, width), f32),
            pltpu.VMEM((3, width), f32),
            pltpu.SemaphoreType.DMA,
            pltpu.SemaphoreType.DMA((3,)),
            pltpu.SemaphoreType.DMA,
            pltpu.SemaphoreType.DMA((3,)),
            pltpu.SemaphoreType.DMA,
            pltpu.SemaphoreType.DMA((2,)),
            pltpu.SemaphoreType.DMA((8,)),
            pltpu.SemaphoreType.DMA((7,)),
            pltpu.SemaphoreType.REGULAR((9,)),
            pltpu.SemaphoreType.REGULAR,
            pltpu.SemaphoreType.REGULAR,
        ],
        compiler_params=pltpu.CompilerParams(collective_id=0, has_side_effects=True, vmem_limit_bytes=60 * 2**20),
        name="inflow",
    )(
        random_slabs.transpose(0, 2, 1, 3),
        wall_filter,
        prev_state.transpose(1, 0, 2),
        span_weights,
        time_scale,
        mean_velocity.reshape(1, -1),
        lund_diag,
        lund_off,
    )
    velocity, state = pl.pallas_call(
        finish,
        out_shape=(
            jax.ShapeDtypeStruct((rows, parts, planes, width), bf16),
            jax.ShapeDtypeStruct((parts, rows, width), f32),
        ),
        in_specs=[pl.BlockSpec(memory_space=pltpu.VMEM)] * 2,
        out_specs=(any_spec, any_spec),
        scratch_shapes=[pltpu.SemaphoreType.DMA((2, 3))],
        compiler_params=pltpu.CompilerParams(vmem_limit_bytes=8 * 2**20),
        name="finish",
    )(pltpu.with_memory_space_constraint(moving, pltpu.VMEM), pltpu.with_memory_space_constraint(shown, pltpu.VMEM))
    return velocity.transpose(0, 2, 1, 3), state.transpose(1, 0, 2)


def solution(mesh):
    placed = (P("span", None, None, None), P(), P(), P("span", None, None), P(), P(), P(), P())
    return jax.shard_map(
        body,
        mesh=mesh,
        in_specs=placed,
        out_specs=(P("span", None, None, None), P("span", None, None)),
        check_vma=False,
    )
```

```python
import jax
import jax.numpy as jnp
from jax import lax
from jax.experimental import pallas as pl
from jax.experimental.pallas import tpu as pltpu
from jax.sharding import PartitionSpec as P

MESH = pl.DeviceIdType.MESH
GROUP = 16
ROWS = 32
LANES = 128
HALF = 256
PEERS = [(0, 1)] + [(sign * far, other) for far in (1, 2, 3) for sign in (1, -1) for other in (0, 1)] + [(4, 0), (4, 1)]


ORDER = (0, 1, 2, 3, 7, 4, 6, 5)
SCOUT = 0


EARLIER = {0: (), 1: (0,), 2: (0, 1), 3: (0, 1, 2), 4: (0, 1, 2, 3), 5: (0, 1, 2, 3, 4, 6), 6: (0, 1, 4, 7), 7: (0, 1)}
RELAY = 8
ENTRY = {
    0: (("wait", 1), 1, ("wait", 2), 2, ("wait", 7), 7, ("wait", 3), 3, ("wait", 6), 6, ("wait", 4), 4, ("wait", 5), 5),
    1: (0, ("wait", 2), 2, ("wait", 3), 3, ("wait", 7), 7, ("wait", 4), 4, ("wait", 6), 6, ("wait", 5), 5),
    2: (1, 0, ("wait", 3), 3, ("wait", 4), 4, ("wait", 5), 5, ("wait", RELAY), 6, 7),
    3: (2, 1, 0, ("wait", 4), 4, ("wait", 5), 5, ("wait", RELAY), 6, 7),
    4: (3, 2, 1, 0, ("wait", 5), ("wait", 6), ("relay", (5, 3, 2)), 5, 6, 7),
    5: (6, 4, 3, 2, 1, 0, ("wait", RELAY), 7),
    6: (7, 4, 0, 1, ("fill", (7, 4)), ("wait", 5), ("relay", (7,)), 5, 2, 3),
    7: (0, 1, ("fill", (0, 1)), ("wait", 6), 6, 4, ("wait", RELAY), 5, 2, 3),
}


def wait_for(view, sem):
    pltpu.make_async_copy(view, view, sem).wait()


def kernel(
    x, wall, prev, weights, scale, mean, diag, off,
    moving, shown,
    held, spread, columns, made, spanned, wide, turned, band, state, carried, sums, mixed,
    vweights, vscale, vmean, vdiag, voff,
    in_send, in_recv, halo_send, halo_recv, out_send, out_recv, last_recv, load_sem, ready, scouts, release,
):
    devices = lax.axis_size("span")
    me = lax.axis_index("span")
    base = (me // GROUP) * GROUP
    pos = lax.rem(me, GROUP)
    chip = pos // 2
    core = lax.rem(pos, 2)

    def place(far, other):
        return lax.rem(chip + far + 8, 8) * 2 + lax.rem(core + other, 2)

    before = lax.rem(me + devices - GROUP, devices)
    after = lax.rem(me + GROUP, devices)

    scout = pos == SCOUT
    barrier = pltpu.get_barrier_semaphore()

    def signal_chip(target, sem):
        for side in (0, 1):
            pl.semaphore_signal(sem, inc=1, device_id=(base + 2 * target + side,), device_id_type=MESH)

    pl.semaphore_signal(barrier, inc=1, device_id=(base + place(0, 1),), device_id_type=MESH)
    for which in range(8):

        @pl.when(chip == which)
        def _():
            for target in ORDER:
                if which in EARLIER[target]:
                    signal_chip(target, barrier)

    @pl.when(scout)
    def _():
        for device in (before, after):
            pl.semaphore_signal(barrier, inc=1, device_id=(device,), device_id_type=MESH)

    loads = []
    for index, (source, target) in enumerate(
        ((weights, vweights), (scale, vscale), (mean, vmean), (diag, vdiag), (off, voff), (prev, state), (wall, wide))
    ):
        loads.append(pltpu.make_async_copy(source, target, load_sem.at[index]))
        loads[-1].start()
    for c in range(3):
        pltpu.make_async_copy(
            x.at[:, c, :, pl.ds(pl.multiple_of(pos * LANES, LANES), LANES)], held.at[c, 8 + pos], in_recv.at[c]
        ).start()

    def send_in(c, there):
        pltpu.make_async_remote_copy(
            src_ref=x.at[:, c, :, pl.ds(pl.multiple_of(there * LANES, LANES), LANES)],
            dst_ref=held.at[c, 8 + pos],
            send_sem=in_send,
            recv_sem=in_recv.at[c],
            device_id=(base + there,),
            device_id_type=MESH,
        ).start()

    @pl.when(scout)
    def _():
        pl.semaphore_wait(barrier, 3)

    for which in range(8):

        @pl.when(jnp.logical_and(chip == which, jnp.logical_not(scout)))
        def _():
            pl.semaphore_wait(barrier, 2 * len(EARLIER[which]) + 1)

        @pl.when(chip == which)
        def _():
            for target in EARLIER[which]:
                signal_chip(target, ready.at[which])
            send_in(0, place(0, 1))
            early = set()
            for step in ENTRY[which]:
                if isinstance(step, int):
                    send_in(0, 2 * step)
                    send_in(0, 2 * step + 1)
                elif step[0] == "wait":
                    pl.semaphore_wait(ready.at[step[1]], 2)
                elif step[0] == "relay":
                    for target in step[1]:
                        signal_chip(target, ready.at[RELAY])
                else:
                    for target in step[1]:
                        send_in(1, 2 * target)
                        send_in(1, 2 * target + 1)
                        early.add(target)
            for far, other in PEERS:
                if (which + far) % 8 not in early:
                    send_in(1, place(far, other))

    for far, other in PEERS:
        send_in(2, place(far, other))

    @pl.when(scout)
    def _():
        for device in (before, after):
            pl.semaphore_signal(scouts, inc=1, device_id=(device,), device_id_type=MESH)

    loads[0].wait()
    taps = vweights[...].reshape(1, 2 * HALF + 1)
    taps = (taps / jnp.sqrt(jnp.sum(taps * taps))).astype(jnp.bfloat16).astype(jnp.float32)
    padded = jnp.concatenate([taps, jnp.zeros((1, 1024 - taps.shape[1]), jnp.float32)], axis=1)
    rolled = pltpu.roll(jnp.broadcast_to(padded, (HALF, 1024)), 0, 1, stride=1, stride_axis=0)
    band[...] = rolled[:, : 3 * HALF].astype(jnp.bfloat16)

    loads[6].wait()
    one = (
        lax.broadcasted_iota(jnp.int32, (256, 256), 0) == lax.broadcasted_iota(jnp.int32, (256, 256), 1)
    ).astype(jnp.bfloat16)

    def turn(step, carry):
        row = pl.multiple_of(step * 256, 256)
        for block in range(8):
            piece = wide[pl.ds(row, 256), block * 256 : (block + 1) * 256]
            turned[block * 256 : (block + 1) * 256, pl.ds(row, 256)] = lax.dot_general(
                one, piece, (((1,), (1,)), ((), ())), preferred_element_type=jnp.float32
            ).astype(jnp.bfloat16)
        return carry

    lax.fori_loop(0, 8, turn, 0)

    for index in range(1, 6):
        loads[index].wait()

    @pl.when(scout)
    def _():
        pl.semaphore_wait(scouts, 2)
        for far, other in PEERS:
            pl.semaphore_signal(release, inc=1, device_id=(base + place(far, other),), device_id_type=MESH)

    @pl.when(jnp.logical_not(scout))
    def _():
        pl.semaphore_wait(release, 1)

    flat = held.reshape(3 * 32 * ROWS * 4, LANES)

    def unpack(c, slot):
        first = pl.multiple_of((c * 32 + slot) * LANES, LANES)
        row = pl.multiple_of(slot * LANES, LANES)
        spread[pl.ds(row, LANES), :] = flat[pl.ds(first, LANES), :].astype(jnp.float32)
        for t in range(4):
            columns[pl.ds(pl.multiple_of(slot * ROWS, ROWS), ROWS), t * LANES : (t + 1) * LANES] = spread[
                pl.ds(row + t, ROWS, stride=4), :
            ].astype(jnp.bfloat16)

    for c in range(3):
        wait_for(held.at[c, pl.ds(8, GROUP)], in_recv.at[c])
        for source, target, device in ((8, 24, before), (16, 0, after)):
            pltpu.make_async_remote_copy(
                src_ref=held.at[c, pl.ds(source, 8)],
                dst_ref=held.at[c, pl.ds(target, 8)],
                send_sem=halo_send,
                recv_sem=halo_recv.at[c],
                device_id=(device,),
                device_id_type=MESH,
            ).start()

        def middle(step, carry):
            for part in range(4):
                unpack(c, 8 + step * 4 + part)
            return carry

        lax.fori_loop(0, 4, middle, 0)
        wait_for(held.at[c, pl.ds(8, GROUP)], halo_recv.at[c])

        def outer(step, carry):
            for part in range(4):
                unpack(c, step * 4 + part)
                unpack(c, 24 + step * 4 + part)
            return carry

        lax.fori_loop(0, 2, outer, 0)
        for half in range(2):
            block = jnp.dot(
                band[...], columns[half * HALF : half * HALF + 3 * HALF, :], preferred_element_type=jnp.float32
            ).astype(jnp.bfloat16)
            for t in range(4):
                made[c, t, half * HALF : (half + 1) * HALF, :] = block[:, t * LANES : (t + 1) * LANES]
        spanned[c, :, :, pl.ds(pl.multiple_of(pos * LANES, LANES), LANES)] = made[
            c, :, pl.ds(pl.multiple_of(pos * ROWS, ROWS), ROWS), :
        ]
        def send_out(there, sem):
            pltpu.make_async_remote_copy(
                src_ref=made.at[c, :, pl.ds(pl.multiple_of(there * ROWS, ROWS), ROWS), :],
                dst_ref=spanned.at[c, :, :, pl.ds(pl.multiple_of(pos * LANES, LANES), LANES)],
                send_sem=out_send,
                recv_sem=sem,
                device_id=(base + there,),
                device_id_type=MESH,
            ).start()

        if c < 2:
            for far, other in PEERS:
                send_out(place(far, other), out_recv.at[c])
        else:
            for target in ORDER:
                for side in (0, 1):

                    @pl.when(pos != 2 * target + side)
                    def _():
                        send_out(2 * target + side, last_recv.at[lax.rem(target - chip + 8, 8)])

    for c in range(3):
        if c < 2:
            wait_for(spanned.at[c, :, :, pl.ds(0, 15 * LANES)], out_recv.at[c])
        for index, far in enumerate((0, 1, -1, 2, -2, 3, -3, 4)):
            if c == 2:
                wait_for(spanned.at[c, :, :, pl.ds(0, 2 * LANES if far else LANES)], last_recv.at[far % 8])
            origin = pl.multiple_of(lax.rem(chip - far + 8, 8) * 256, 256)
            piece = spanned[c, :, :, pl.ds(origin, 256)].reshape(4 * ROWS, 256)
            term = jnp.dot(piece, turned[pl.ds(origin, 256), :], preferred_element_type=jnp.float32)
            if index == 0:
                sums[...] = term
            else:
                sums[...] += term
        for block in range(8):
            cols = slice(block * 256, (block + 1) * 256)
            time = vscale[c : c + 1, cols]
            decay = jnp.exp(-jnp.pi / (2.0 * time))
            inject = jnp.sqrt(1.0 - jnp.exp(-jnp.pi / time))
            value = state[c, :, cols]
            for t in range(4):
                value = decay * value + inject * sums[t * ROWS : (t + 1) * ROWS, cols]
                if c == 0:
                    carried[0, t, :, cols] = value
                    out = vmean[:, cols] + vdiag[0:1, cols] * value
                elif c == 1:
                    along = carried[0, t, :, cols]
                    out = voff[0:1, cols] * along + vdiag[1:2, cols] * value
                    carried[0, t, :, cols] = voff[1:2, cols] * along + voff[2:3, cols] * value
                else:
                    out = carried[0, t, :, cols] + vdiag[2:3, cols] * value
                for side in range(2):
                    mixed[2 * block + side, pl.ds(t, ROWS, stride=4), :] = out[:, side * LANES : (side + 1) * LANES]
            shown[c, :, cols] = value
            for tile in (2 * block, 2 * block + 1):
                moving[c, :, :, tile * LANES : (tile + 1) * LANES] = (
                    mixed[tile].reshape(ROWS, 4, LANES).astype(jnp.bfloat16)
                )

    wait_for(x.at[:, :, :, pl.ds(0, 15 * LANES)], in_send)
    wait_for(held.at[:, pl.ds(0, GROUP)], halo_send)
    wait_for(made.at[:, :, pl.ds(0, 15 * ROWS), :], out_send)


def finish(moving, shown, velocity, final, sems):
    copies = []
    for c in range(3):
        copies.append(pltpu.make_async_copy(moving.at[c], velocity.at[:, c], sems.at[0, c]))
        copies.append(pltpu.make_async_copy(shown.at[c], final.at[c], sems.at[1, c]))
    for copy in copies:
        copy.start()
    for copy in copies:
        copy.wait()


def body(random_slabs, span_weights, wall_filter, prev_state, time_scale, mean_velocity, lund_diag, lund_off):
    rows, planes, parts, width = random_slabs.shape
    any_spec = pl.BlockSpec(memory_space=pl.ANY)
    bf16, f32 = jnp.bfloat16, jnp.float32
    moving, shown = pl.pallas_call(
        kernel,
        out_shape=(
            pltpu.VMEM((parts, rows, planes, width), bf16),
            pltpu.VMEM((parts, rows, width), f32),
        ),
        in_specs=[any_spec] * 8,
        out_specs=(pl.BlockSpec(memory_space=pltpu.VMEM),) * 2,
        scratch_shapes=[
            pltpu.VMEM((3, 32, ROWS, 4, LANES), bf16),
            pltpu.VMEM((4096, LANES), f32),
            pltpu.VMEM((1024, 4 * LANES), bf16),
            pltpu.VMEM((3, 4, 512, LANES), bf16),
            pltpu.VMEM((3, 4, ROWS, width), bf16),
            pltpu.VMEM((width, width), bf16),
            pltpu.VMEM((width, width), bf16),
            pltpu.VMEM((HALF, 3 * HALF), bf16),
            pltpu.VMEM((3, ROWS, width), f32),
            pltpu.VMEM((1, 4, ROWS, width), f32),
            pltpu.VMEM((4 * ROWS, width), f32),
            pltpu.VMEM((width // LANES, 4 * ROWS, LANES), f32),
            pltpu.VMEM((2 * HALF + 1,), f32),
            pltpu.VMEM((3, width), f32),
            pltpu.VMEM((1, width), f32),
            pltpu.VMEM((3, width), f32),
            pltpu.VMEM((3, width), f32),
            pltpu.SemaphoreType.DMA,
            pltpu.SemaphoreType.DMA((3,)),
            pltpu.SemaphoreType.DMA,
            pltpu.SemaphoreType.DMA((3,)),
            pltpu.SemaphoreType.DMA,
            pltpu.SemaphoreType.DMA((2,)),
            pltpu.SemaphoreType.DMA((8,)),
            pltpu.SemaphoreType.DMA((7,)),
            pltpu.SemaphoreType.REGULAR((9,)),
            pltpu.SemaphoreType.REGULAR,
            pltpu.SemaphoreType.REGULAR,
        ],
        compiler_params=pltpu.CompilerParams(collective_id=0, has_side_effects=True, vmem_limit_bytes=60 * 2**20),
        name="inflow",
    )(
        random_slabs.transpose(0, 2, 1, 3),
        wall_filter,
        prev_state.transpose(1, 0, 2),
        span_weights,
        time_scale,
        mean_velocity.reshape(1, -1),
        lund_diag,
        lund_off,
    )
    velocity, state = pl.pallas_call(
        finish,
        out_shape=(
            jax.ShapeDtypeStruct((rows, parts, planes, width), bf16),
            jax.ShapeDtypeStruct((parts, rows, width), f32),
        ),
        in_specs=[pl.BlockSpec(memory_space=pltpu.VMEM)] * 2,
        out_specs=(any_spec, any_spec),
        scratch_shapes=[pltpu.SemaphoreType.DMA((2, 3))],
        compiler_params=pltpu.CompilerParams(vmem_limit_bytes=8 * 2**20),
        name="finish",
    )(pltpu.with_memory_space_constraint(moving, pltpu.VMEM), pltpu.with_memory_space_constraint(shown, pltpu.VMEM))
    return velocity.transpose(0, 2, 1, 3), state.transpose(1, 0, 2)


def solution(mesh):
    placed = (P("span", None, None, None), P(), P(), P("span", None, None), P(), P(), P(), P())
    return jax.shard_map(
        body,
        mesh=mesh,
        in_specs=placed,
        out_specs=(P("span", None, None, None), P("span", None, None)),
        check_vma=False,
    )
```
